32 devices in a mesh: gx: 4 (over y, x), gy: 8 (over z, core).
Axes of the slice: x: 2, y: 2, z: 4, core: 2. Of those that a mesh axis runs over, the one named last changes fastest.
Arguments:
- value_field: float32 [4, 24, 48, 1536], P(None, 'gx', 'gy'), may hold values from -16 to 17
- target_mask: int32 [4, 24, 48, 1536], P(None, 'gx', 'gy'), may hold values 0 or 1
- obstacle_mask: int32 [4, 24, 48, 1536], P(None, 'gx', 'gy'), may hold values 0 or 1
- drift_gains: float32 [5], replicated, may hold values from 0.5 to 2
- control_costs: float32 [5], replicated, may hold values from 0.25 to 1
Outputs:
- reach_value: float32 [4, 24, 48, 1536], P(None, 'gx', 'gy')
- time_steps: float32 [3], replicated
The draws below stay inside these ranges and needn't reach their ends.
All inputs are finite; a program needn't handle non-finite values. No bound on the sum of `target_mask` or of `obstacle_mask` on one device may be relied on, other than what follows from the above.
Results may differ from the reference program's by a relative error of at most 0.0003.
Values sent between devices are 32-bit elements; how exact they have to be, the bound alone decides.
A program may use at most 128 MiB of HBM per device.

```python
import math
import jax
import jax.numpy as jnp
from jax import lax

PLANES = 4
N3 = 32
N4 = 48
GRID = 96
STEPS = 3
NA = 24
NB = 48


def draw_value_field(key, part):
    base_key = jax.random.fold_in(key, 11)
    rough_key, row_key, col_key = jax.random.split(base_key, 3)
    grid_shape = (PLANES, NA, NB, N3 * N4)
    rough_part = jnp.clip(jax.random.normal(rough_key, grid_shape, jnp.float32), -4.0, 4.0)
    row_scale = jnp.exp(jax.random.uniform(row_key, (NA,), jnp.float32, -math.log(2.0), math.log(2.0)))
    col_scale = jnp.exp(jax.random.uniform(col_key, (NB,), jnp.float32, -math.log(2.0), math.log(2.0)))
    return rough_part * row_scale[None, :, None, None] * col_scale[None, None, :, None]


def with_ends(values, own_key, smallest, largest):
    place = [jax.random.randint(jax.random.fold_in(own_key, axis), (), 0, length) for axis, length in enumerate(values.shape)]
    main_axis = values.shape.index(max(values.shape))
    neighbour = place[:main_axis] + [(place[main_axis] + 1) % values.shape[main_axis]] + place[main_axis + 1:]
    return values.at[tuple(place)].set(smallest).at[tuple(neighbour)].set(largest)


def setup_inputs(seed: int = 0) -> dict:
    splits = jax.random.split(jax.random.key(seed), 6)
    return {
        "value_field": draw_value_field(jax.random.fold_in(splits[5], 71), 0),
        "target_mask": with_ends((jax.random.randint(splits[1], (PLANES, NA, NB, N3 * N4), 0, 4) < 1).astype(jnp.int32), jax.random.fold_in(splits[1], 1), 0, 1),
        "obstacle_mask": with_ends((jax.random.randint(splits[2], (PLANES, NA, NB, N3 * N4), 0, 5) < 1).astype(jnp.int32), jax.random.fold_in(splits[2], 1), 0, 1),
        "drift_gains": jnp.clip(jnp.exp(jax.random.uniform(splits[3], (5,), jnp.float32, math.log(0.5), math.log(2.0))), 0.5, 2.0),
        "control_costs": jnp.clip(jnp.exp(jax.random.uniform(splits[4], (5,), jnp.float32, math.log(0.25), math.log(1.0))), 0.25, 1.0),
    }


courant = 0.5
weno_eps = 1e-6


def weno_side(diff_one, diff_two, diff_three, diff_four, diff_five):
    stencil_one = diff_one / 3.0 - 7.0 * diff_two / 6.0 + 11.0 * diff_three / 6.0
    stencil_two = -diff_two / 6.0 + 5.0 * diff_three / 6.0 + diff_four / 3.0
    stencil_three = diff_three / 3.0 + 5.0 * diff_four / 6.0 - diff_five / 6.0
    smooth_one = 13.0 / 12.0 * (diff_one - 2.0 * diff_two + diff_three) ** 2 + 0.25 * (diff_one - 4.0 * diff_two + 3.0 * diff_three) ** 2
    smooth_two = 13.0 / 12.0 * (diff_two - 2.0 * diff_three + diff_four) ** 2 + 0.25 * (diff_two - diff_four) ** 2
    smooth_three = 13.0 / 12.0 * (diff_three - 2.0 * diff_four + diff_five) ** 2 + 0.25 * (3.0 * diff_three - 4.0 * diff_four + diff_five) ** 2
    weight_one = 0.1 / (weno_eps + smooth_one) ** 2
    weight_two = 0.6 / (weno_eps + smooth_two) ** 2
    weight_three = 0.3 / (weno_eps + smooth_three) ** 2
    return (weight_one * stencil_one + weight_two * stencil_two + weight_three * stencil_three) / (weight_one + weight_two + weight_three)


def axis_slopes(shifted, spacing):
    differences = [shifted[offset + 1] - shifted[offset] for offset in range(6)]
    minus_slope = weno_side(differences[0], differences[1], differences[2], differences[3], differences[4]) / spacing
    plus_slope = weno_side(differences[5], differences[4], differences[3], differences[2], differences[1]) / spacing
    return minus_slope, plus_slope


def merged_shifts(interior, stride, position, extent):
    upward = []
    current = interior
    for offset in range(1, 4):
        current = jnp.where(position + offset <= extent - 1, jnp.roll(interior, -offset * stride, axis=-1), current)
        upward.append(current)
    downward = []
    current = interior
    for offset in range(1, 4):
        current = jnp.where(position - offset >= 0, jnp.roll(interior, offset * stride, axis=-1), current)
        downward.append(current)
    return [downward[2], downward[1], downward[0], interior, upward[0], upward[1], upward[2]]


def drift_field(first_pos, heading_one, heading_two, third_pos, fourth_pos, drift_gains):
    return [drift_gains[0] * (jnp.cos(heading_one) - 0.5 * jnp.cos(heading_two) + third_pos),
            drift_gains[1] * (fourth_pos - 0.3 * first_pos),
            drift_gains[2] * (third_pos + 0.5 * jnp.sin(heading_one)),
            drift_gains[3] * (jnp.sin(heading_two) - first_pos),
            drift_gains[4] * (jnp.cos(heading_one) * jnp.sin(heading_two) - fourth_pos)]


def local_bounds(drift_terms, slopes, control_costs, spacing_list):
    peaks = []
    for axis_number in range(5):
        scale = control_costs[axis_number] * spacing_list[axis_number]
        minus_peak = jnp.max(jnp.abs(drift_terms[axis_number] - scale * slopes[axis_number][0]))
        plus_peak = jnp.max(jnp.abs(drift_terms[axis_number] - scale * slopes[axis_number][1]))
        peaks.append(jnp.maximum(minus_peak, plus_peak))
    return jnp.stack(peaks)


def advance(interior, slopes, drift_terms, bounds, time_step, control_costs, spacing_list, target_plane, obstacle_plane):
    hamiltonian = jnp.zeros_like(interior)
    for axis_number in range(5):
        minus_slope, plus_slope = slopes[axis_number]
        middle = 0.5 * (minus_slope + plus_slope)
        hamiltonian = hamiltonian + drift_terms[axis_number] * middle - 0.5 * control_costs[axis_number] * spacing_list[axis_number] * middle * middle
        hamiltonian = hamiltonian - bounds[axis_number] * 0.5 * (plus_slope - minus_slope)
    advanced = interior - time_step * hamiltonian
    advanced = jnp.where(target_plane == 1, jnp.minimum(advanced, -0.5), advanced)
    return jnp.where(obstacle_plane == 1, jnp.maximum(advanced, 0.5), advanced)


def plane_state(padded, plane_index, drift_gains, spacing_list):
    center = lax.dynamic_index_in_dim(padded, plane_index, 0, keepdims=False)
    interior = center[3:-3, 3:-3]
    neighbours = [lax.dynamic_index_in_dim(padded, jnp.clip(plane_index + offset - 3, 0, PLANES - 1).astype(jnp.int32), 0, keepdims=False)[3:-3, 3:-3] for offset in range(7)]
    row_shifts = [center[offset:offset + NA, 3:-3] for offset in range(7)]
    col_shifts = [center[3:-3, offset:offset + NB] for offset in range(7)]
    lane_index = jnp.arange(N3 * N4, dtype=jnp.int32)
    slopes = [axis_slopes(neighbours, spacing_list[0]),
              axis_slopes(row_shifts, spacing_list[1]),
              axis_slopes(col_shifts, spacing_list[2]),
              axis_slopes(merged_shifts(interior, N4, lane_index // N4, N3), spacing_list[3]),
              axis_slopes(merged_shifts(interior, 1, lane_index % N4, N4), spacing_list[4])]
    first_pos = (plane_index.astype(jnp.float32) - PLANES / 2 + 0.5) * (2.0 / GRID)
    heading_one = ((2.0 * math.pi / NA) * jnp.arange(NA, dtype=jnp.float32)).reshape(NA, 1, 1)
    heading_two = ((2.0 * math.pi / NB) * jnp.arange(NB, dtype=jnp.float32)).reshape(1, NB, 1)
    third_pos = (((lane_index // N4).astype(jnp.float32) - N3 / 2 + 0.5) * (2.0 / GRID)).reshape(1, 1, -1)
    fourth_pos = (((lane_index % N4).astype(jnp.float32) - N4 / 2 + 0.5) * (2.0 / GRID)).reshape(1, 1, -1)
    drift_terms = drift_field(first_pos, heading_one, heading_two, third_pos, fourth_pos, drift_gains)
    return interior, slopes, drift_terms


def reference(value_field, target_mask, obstacle_mask, drift_gains, control_costs):
    spacing_list = [2.0 / GRID, 2.0 * math.pi / NA, 2.0 * math.pi / NB, 2.0 / GRID, 2.0 / GRID]
    spacing_array = jnp.array(spacing_list, dtype=jnp.float32)
    plane_ids = jnp.arange(PLANES, dtype=jnp.int32)
    value_now = value_field
    step_sizes = []
    for section_number in range(STEPS):
        padded = jnp.pad(value_now, ((0, 0), (3, 3), (3, 3), (0, 0)), mode="wrap")

        def bound_plane(plane_index):
            interior, slopes, drift_terms = plane_state(padded, plane_index, drift_gains, spacing_list)
            return local_bounds(drift_terms, slopes, control_costs, spacing_list)

        bounds = jnp.max(lax.map(bound_plane, plane_ids), axis=0)
        time_step = courant / (jnp.sum(bounds / spacing_array) + 1e-6)

        def move_plane(items):
            plane_index, target_plane, obstacle_plane = items
            interior, slopes, drift_terms = plane_state(padded, plane_index, drift_gains, spacing_list)
            return advance(interior, slopes, drift_terms, bounds, time_step, control_costs, spacing_list, target_plane, obstacle_plane)

        value_now = lax.map(move_plane, (plane_ids, target_mask, obstacle_mask))
        step_sizes.append(time_step)
    return value_now, jnp.stack(step_sizes)
```

```python
import functools
import math

import jax
import jax.numpy as jnp
from jax import lax
from jax.experimental import pallas as pl
from jax.experimental.pallas import tpu as pltpu
from jax.sharding import PartitionSpec as P

N3 = 32
N4 = 48
GRID = 96
STEPS = 3
COURANT = 0.5
EPS = 0.75e-6
LANES = 8 * N4


def wave(vs):
    n = len(vs) - 6
    d = [vs[k + 1] - vs[k] for k in range(n + 5)]
    f = [d[k + 1] - d[k] for k in range(n + 4)]
    e = [f[k + 1] - f[k] for k in range(n + 3)]
    j = [e[k + 1] - e[k] for k in range(n + 2)]
    k15 = [1.5 * x for x in f]
    base = [e[k] * e[k] + (0.5 * k15[k] * f[k + 1] + EPS) for k in range(n + 3)]
    left, mid, right = [], [], []
    for k in range(n + 1):
        a = base[k] + k15[k + 1] * e[k]
        b = base[k + 1]
        c = base[k + 2] - k15[k + 2] * e[k + 2]
        left.append(a * a)
        mid.append(b * b)
        right.append(c * c)
    low, high = [], []
    for k in range(n + 1):
        bc = mid[k] * right[k]
        ab = left[k] * mid[k]
        ac = 6.0 * (left[k] * right[k])
        n1 = bc * j[k]
        n2 = ab * j[k + 1]
        total = bc + ab
        both = n1 + n2
        both = both + both
        core = total + ac
        low.append((both + n2) / (core + (ab + ab)) if k < n else None)
        high.append((both + n1) / (core + (bc + bc)) if k > 0 else None)
    out = []
    for i in range(n):
        rm, rp = low[i], high[i + 1]
        center = 6.0 * (vs[i + 4] - vs[i + 2])
        middle = center - (e[i + 1] + e[i + 2]) + (rp - rm)
        jump = (rp + rm) - j[i + 1]
        out.append((middle, jump))
    return out


def tally(middle, jump, drift, kappa):
    gap = drift - middle
    return jnp.abs(gap) + jnp.abs(jump), (kappa * middle) * (drift + gap)


def unsplit_kernel(kappa_ref, v_ref, f0_ref, f3_ref, f4_ref, h_ref, q_ref, peak_ref, up_ref):
    planes, rows, cols, width = v_ref.shape
    lane = lax.broadcasted_iota(jnp.int32, (1, width), 1)
    third, fourth = lane // N4, lane % N4
    peak_ref[...] = jnp.zeros_like(peak_ref)

    def per_row(r, carry):
        def shift(p, carry):
            v = v_ref[p, r]
            for base, stride, place, extent in ((0, N4, third, width // N4), (6, 1, fourth, N4)):
                now = v
                for s in range(1, 4):
                    now = jnp.where(place + s < extent, pltpu.roll(v, width - s * stride, 1), now)
                    up_ref[base + 2 + s, p] = now
                now = v
                for s in range(1, 4):
                    now = jnp.where(place >= s, pltpu.roll(v, s * stride, 1), now)
                    up_ref[base + 3 - s, p] = now
            return carry

        lax.fori_loop(0, planes, shift, 0)

        def per_group(g, carry):
            at = pl.ds(pl.multiple_of(g * LANES, 128), LANES)
            vs = [v_ref[p, r, :, at] for p in range(planes)]
            drift = f0_ref[r, :, at]
            top = peak_ref[0]
            cells = wave([vs[0]] * 3 + vs + [vs[-1]] * 3)
            for p in range(planes):
                speed, part = tally(*cells[p], drift, kappa_ref[0])
                top = jnp.maximum(top, speed)
                h_ref[p, r, :, at] = part
                q_ref[0, p, r, :, at] = cells[p][1]
            peak_ref[0] = top

            def per_plane(p, carry):
                v = v_ref[p, r, :, at]
                total = h_ref[p, r, :, at]
                for slot, base, number in ((1, 0, 3), (2, 6, 4)):
                    around = [up_ref[base + k, p, :, at] for k in range(6)]
                    ((middle, jump),) = wave(around[:3] + [v] + around[3:])
                    drift = f3_ref[p, :, :] if number == 3 else f4_ref[r, :, at]
                    speed, part = tally(middle, jump, drift, kappa_ref[number])
                    peak_ref[slot] = jnp.maximum(peak_ref[slot], speed)
                    q_ref[slot, p, r, :, at] = jump
                    total = total + part
                h_ref[p, r, :, at] = total
                return carry

            lax.fori_loop(0, planes, per_plane, 0)
            return carry

        lax.fori_loop(0, width // LANES, per_group, 0)
        return carry

    lax.fori_loop(0, rows, per_row, 0)


def split_kernel(
    kappa_ref, v_ref, a_lo, a_hi, b_lo, b_hi, f1_ref, f2_ref, hin_ref, h_ref, q_ref, peak_ref, ext_ref
):
    planes, rows, cols, width = v_ref.shape
    peak_ref[...] = jnp.zeros_like(peak_ref)

    def per_plane(p, carry):
        def fill(r, carry):
            ext_ref[r, 0:3, :] = b_lo[p, r]
            ext_ref[r, 3 : 3 + cols, :] = v_ref[p, r]
            ext_ref[r, 3 + cols : 6 + cols, :] = b_hi[p, r]
            return carry

        lax.fori_loop(0, rows, fill, 0)

        def per_group(g, carry):
            at = pl.ds(pl.multiple_of(g * LANES, 128), LANES)
            vs = [a_lo[p, k, :, at] for k in range(3)]
            vs += [v_ref[p, r, :, at] for r in range(rows)]
            vs += [a_hi[p, k, :, at] for k in range(3)]
            top = peak_ref[0]
            drift = f1_ref[p, :, at]
            for r, (middle, jump) in enumerate(wave(vs)):
                speed, part = tally(middle, jump, drift, kappa_ref[1])
                top = jnp.maximum(top, speed)
                h_ref[p, r, :, at] = hin_ref[p, r, :, at] + part
                q_ref[0, p, r, :, at] = jump
            peak_ref[0] = top

            def per_row(r, carry):
                around = [ext_ref[r, k : k + cols, at] for k in range(7)]
                ((middle, jump),) = wave(around)
                speed, part = tally(middle, jump, f2_ref[r, :, at], kappa_ref[2])
                peak_ref[1] = jnp.maximum(peak_ref[1], speed)
                h_ref[p, r, :, at] = h_ref[p, r, :, at] + part
                q_ref[1, p, r, :, at] = jump
                return carry

            lax.fori_loop(0, rows, per_row, 0)
            return carry

        lax.fori_loop(0, width // LANES, per_group, 0)
        return carry

    lax.fori_loop(0, planes, per_plane, 0)


def move_kernel(scale_ref, v_ref, h_ref, qu_ref, qs_ref, target_ref, obstacle_ref, out_ref):
    planes, rows, cols, width = v_ref.shape

    def per_cell(i, carry):
        p, r = i // rows, i % rows
        change = scale_ref[0] * h_ref[p, r]
        change = change - scale_ref[1] * qu_ref[0, p, r] - scale_ref[2] * qs_ref[0, p, r]
        change = change - scale_ref[3] * qs_ref[1, p, r] - scale_ref[4] * qu_ref[1, p, r]
        change = change - scale_ref[5] * qu_ref[2, p, r]
        new = v_ref[p, r] - change
        new = jnp.where(target_ref[p, r] == 1, jnp.minimum(new, -0.5), new)
        out_ref[p, r] = jnp.where(obstacle_ref[p, r] == 1, jnp.maximum(new, 0.5), new)
        return carry

    lax.fori_loop(0, planes * rows, per_cell, 0)


VMEM = pl.BlockSpec(memory_space=pltpu.VMEM)
SMEM = pl.BlockSpec(memory_space=pltpu.SMEM)


def call(kernel, ins, outs, scratch, flops, args):
    return pl.pallas_call(
        kernel,
        out_shape=[jax.ShapeDtypeStruct(s, jnp.float32) for s in outs],
        in_specs=[SMEM] + [VMEM] * ins,
        out_specs=[VMEM] * len(outs),
        scratch_shapes=scratch,
        cost_estimate=pl.CostEstimate(flops=flops, bytes_accessed=1 << 20, transcendentals=0),
        compiler_params=pltpu.CompilerParams(vmem_limit_bytes=40 << 20),
    )(*args)


def drifts(shape, gains):
    planes, rows, cols, width = shape
    one = 2.0 * math.pi / (rows * lax.axis_size("gx"))
    two = 2.0 * math.pi / (cols * lax.axis_size("gy"))
    row = lax.axis_index("gx") * rows + jnp.arange(rows, dtype=jnp.int32)
    col = lax.axis_index("gy") * cols + jnp.arange(cols, dtype=jnp.int32)
    first = (jnp.arange(planes, dtype=jnp.float32) - planes / 2 + 0.5) * (2.0 / GRID)
    a = (one * row.astype(jnp.float32)).reshape(rows, 1, 1)
    b = (two * col.astype(jnp.float32)).reshape(1, cols, 1)
    lane = jnp.arange(width, dtype=jnp.int32)
    third = ((lane // N4).astype(jnp.float32) - N3 / 2 + 0.5) * (2.0 / GRID)
    fourth = ((lane % N4).astype(jnp.float32) - N4 / 2 + 0.5) * (2.0 / GRID)
    third, fourth = third.reshape(1, 1, -1), fourth.reshape(1, 1, -1)
    x0 = first.reshape(planes, 1, 1)
    f3 = gains[3] * (jnp.sin(b) - x0)
    return [
        gains[0] * (jnp.cos(a) - 0.5 * jnp.cos(b) + third),
        gains[1] * (fourth - 0.3 * x0),
        gains[2] * (third + 0.5 * jnp.sin(a)),
        jnp.broadcast_to(f3, (planes, cols, LANES)),
        gains[4] * (jnp.cos(a) * jnp.sin(b) - fourth),
    ]


def exchange(part_lo, part_hi, axis):
    devices = lax.axis_size(axis)
    up = [(i, (i + 1) % devices) for i in range(devices)]
    down = [(k, i) for i, k in up]
    return lax.ppermute(part_hi, axis, up), lax.ppermute(part_lo, axis, down)


def body(value, target, obstacle, gains, costs):
    shape = value.shape
    planes, rows, cols, width = shape
    h = jnp.array(
        [
            2.0 / GRID,
            2.0 * math.pi / (rows * lax.axis_size("gx")),
            2.0 * math.pi / (cols * lax.axis_size("gy")),
            2.0 / GRID,
            2.0 / GRID,
        ],
        dtype=jnp.float32,
    )
    kappa = costs / (288.0 * h)
    f = [d * (12.0 / costs[i]) for i, d in enumerate(drifts(shape, gains))]
    wide = (cols, LANES)
    steps = []
    for _ in range(STEPS):
        a_lo, a_hi = exchange(value[:, :3], value[:, -3:], "gx")
        b_lo, b_hi = exchange(value[:, :, :3], value[:, :, -3:], "gy")
        part, q_un, peak_un = call(
            unsplit_kernel,
            4,
            [shape, (3,) + shape, (3,) + wide],
            [pltpu.VMEM((12, planes, cols, width), jnp.float32)],
            1 << 28,
            (kappa, value, f[0], f[3], f[4]),
        )
        part, q_sp, peak_sp = call(
            split_kernel,
            8,
            [shape, (2,) + shape, (2,) + wide],
            [pltpu.VMEM((rows, cols + 6, width), jnp.float32)],
            1 << 27,
            (kappa, value, a_lo, a_hi, b_lo, b_hi, f[1], f[2], part),
        )
        top_un = jnp.max(peak_un, axis=(1, 2))
        top_sp = jnp.max(peak_sp, axis=(1, 2))
        top = jnp.stack([top_un[0], top_sp[0], top_sp[1], top_un[1], top_un[2]])
        bounds = lax.pmax(top, ("gx", "gy")) * (costs / 12.0)
        dt = COURANT / (jnp.sum(bounds / h) + 1e-6)
        scales = jnp.concatenate([dt[None], dt * bounds / (12.0 * h)])
        (value,) = call(
            move_kernel, 6, [shape], [], 1 << 24,
            (scales, value, part, q_un, q_sp, target, obstacle),
        )
        steps.append(dt)
    return value, jnp.stack(steps)


def solution(mesh):
    spec = P(None, "gx", "gy", None)
    return jax.shard_map(
        body,
        mesh=mesh,
        in_specs=(spec, spec, spec, P(), P()),
        out_specs=(spec, P()),
        check_vma=False,
    )
```

```python
import functools
import math

import jax
import jax.numpy as jnp
from jax import lax
from jax.experimental import pallas as pl
from jax.experimental.pallas import tpu as pltpu
from jax.sharding import PartitionSpec as P

N3 = 32
N4 = 48
GRID = 96
STEPS = 3
COURANT = 0.5
EPS = 0.75e-6
LANES = 8 * N4


def wave(vs):
    n = len(vs) - 6
    d = [vs[k + 1] - vs[k] for k in range(n + 5)]
    f = [d[k + 1] - d[k] for k in range(n + 4)]
    e = [f[k + 1] - f[k] for k in range(n + 3)]
    j = [e[k + 1] - e[k] for k in range(n + 2)]
    k15 = [1.5 * x for x in f]
    base = [e[k] * e[k] + (0.5 * k15[k] * f[k + 1] + EPS) for k in range(n + 3)]
    left, mid, right = [], [], []
    for k in range(n + 1):
        a = base[k] + k15[k + 1] * e[k]
        b = base[k + 1]
        c = base[k + 2] - k15[k + 2] * e[k + 2]
        left.append(a * a)
        mid.append(b * b)
        right.append(c * c)
    low, high = [], []
    for k in range(n + 1):
        bc = mid[k] * right[k]
        ab = left[k] * mid[k]
        ac = 6.0 * (left[k] * right[k])
        n1 = bc * j[k]
        n2 = ab * j[k + 1]
        total = bc + ab
        both = n1 + n2
        both = both + both
        core = total + ac
        low.append((both + n2) / (core + (ab + ab)) if k < n else None)
        high.append((both + n1) / (core + (bc + bc)) if k > 0 else None)
    out = []
    for i in range(n):
        rm, rp = low[i], high[i + 1]
        center = 6.0 * (vs[i + 4] - vs[i + 2])
        middle = center - (e[i + 1] + e[i + 2]) + (rp - rm)
        jump = (rp + rm) - j[i + 1]
        out.append((middle, jump))
    return out


def tally(middle, jump, drift, kappa):
    gap = drift - middle
    return jnp.abs(gap) + jnp.abs(jump), (kappa * middle) * (drift + gap)


def unsplit_kernel(kappa_ref, v_ref, f0_ref, f3_ref, f4_ref, h_ref, q_ref, peak_ref, up_ref):
    planes, rows, cols, width = v_ref.shape
    lane = lax.broadcasted_iota(jnp.int32, (1, width), 1)
    third, fourth = lane // N4, lane % N4
    peak_ref[...] = jnp.zeros_like(peak_ref)

    def per_row(r, carry):
        def shift(p, carry):
            v = v_ref[p, r]
            for base, stride, place, extent in ((0, N4, third, width // N4), (6, 1, fourth, N4)):
                now = v
                for s in range(1, 4):
                    now = jnp.where(place + s < extent, pltpu.roll(v, width - s * stride, 1), now)
                    up_ref[base + 2 + s, p] = now
                now = v
                for s in range(1, 4):
                    now = jnp.where(place >= s, pltpu.roll(v, s * stride, 1), now)
                    up_ref[base + 3 - s, p] = now
            return carry

        lax.fori_loop(0, planes, shift, 0)

        def along_planes(g, carry):
            at = pl.ds(pl.multiple_of(g * 128, 128), 128)
            vs = [v_ref[p, r, :, at] for p in range(planes)]
            drift = f0_ref[r, :, at]
            top = peak_ref[0, :, at]
            cells = wave([vs[0]] * 3 + vs + [vs[-1]] * 3)
            for p in range(planes):
                speed, part = tally(*cells[p], drift, kappa_ref[0])
                top = jnp.maximum(top, speed)
                h_ref[p, r, :, at] = part
                q_ref[0, p, r, :, at] = cells[p][1]
            peak_ref[0, :, at] = top
            return carry

        lax.fori_loop(0, width // 128, along_planes, 0)

        def per_group(g, carry):
            at = pl.ds(pl.multiple_of(g * LANES, 128), LANES)

            def per_plane(p, carry):
                v = v_ref[p, r, :, at]
                total = h_ref[p, r, :, at]
                for slot, base, number in ((1, 0, 3), (2, 6, 4)):
                    around = [up_ref[base + k, p, :, at] for k in range(6)]
                    ((middle, jump),) = wave(around[:3] + [v] + around[3:])
                    drift = f3_ref[p, :, :] if number == 3 else f4_ref[r, :, at]
                    speed, part = tally(middle, jump, drift, kappa_ref[number])
                    peak_ref[slot, :, at] = jnp.maximum(peak_ref[slot, :, at], speed)
                    q_ref[slot, p, r, :, at] = jump
                    total = total + part
                h_ref[p, r, :, at] = total
                return carry

            lax.fori_loop(0, planes, per_plane, 0)
            return carry

        lax.fori_loop(0, width // LANES, per_group, 0)
        return carry

    lax.fori_loop(0, rows, per_row, 0)


def split_kernel(
    kappa_ref, v_ref, a_lo, a_hi, b_lo, b_hi, f1_ref, f2_ref, hin_ref, peak_un_ref,
    h_ref, q_ref, top_ref, ext_ref, near_ref, peak_ref,
):
    planes, rows, cols, width = v_ref.shape
    peak_ref[...] = jnp.zeros_like(peak_ref)

    def per_plane(p, carry):
        def fill(r, carry):
            ext_ref[0:3, :] = b_lo[p, r]
            ext_ref[3 : 3 + cols, :] = v_ref[p, r]
            ext_ref[3 + cols : 6 + cols, :] = b_hi[p, r]
            for k in range(7):
                near_ref[k, r] = ext_ref[k : k + cols, :]
            return carry

        lax.fori_loop(0, rows, fill, 0)

        def along_rows(g, carry):
            at = pl.ds(pl.multiple_of(g * 128, 128), 128)
            vs = [a_lo[p, k, :, at] for k in range(3)]
            vs += [v_ref[p, r, :, at] for r in range(rows)]
            vs += [a_hi[p, k, :, at] for k in range(3)]
            top = peak_ref[0, :, at]
            drift = f1_ref[p, :, at]
            for r, (middle, jump) in enumerate(wave(vs)):
                speed, part = tally(middle, jump, drift, kappa_ref[1])
                top = jnp.maximum(top, speed)
                h_ref[p, r, :, at] = hin_ref[p, r, :, at] + part
                q_ref[0, p, r, :, at] = jump
            peak_ref[0, :, at] = top
            return carry

        lax.fori_loop(0, width // 128, along_rows, 0)

        def per_group(g, carry):
            at = pl.ds(pl.multiple_of(g * LANES, 128), LANES)

            def per_row(r, carry):
                ((middle, jump),) = wave([near_ref[k, r, :, at] for k in range(7)])
                speed, part = tally(middle, jump, f2_ref[r, :, at], kappa_ref[2])
                peak_ref[1, :, at] = jnp.maximum(peak_ref[1, :, at], speed)
                h_ref[p, r, :, at] = h_ref[p, r, :, at] + part
                q_ref[1, p, r, :, at] = jump
                return carry

            lax.fori_loop(0, rows, per_row, 0)
            return carry

        lax.fori_loop(0, width // LANES, per_group, 0)
        return carry

    lax.fori_loop(0, planes, per_plane, 0)
    tops = [peak_un_ref[0], peak_ref[0], peak_ref[1], peak_un_ref[1], peak_un_ref[2]]
    row = lax.broadcasted_iota(jnp.int32, top_ref.shape, 0)
    out = jnp.zeros(top_ref.shape, jnp.float32)
    for number, part in enumerate(tops):
        out = jnp.where(row == number, jnp.max(part), out)
    top_ref[...] = out


def peak_kernel(sizes, own_ref, out_ref, slots, send_sem, recv_sem):
    nx, ny = sizes
    n = nx * ny
    me = lax.axis_index("gx") * ny + lax.axis_index("gy")

    def place(k):
        other = (me + k) % n
        return (other // ny, other % ny)

    barrier = pltpu.get_barrier_semaphore()

    def greet(k, carry):
        pl.semaphore_signal(
            barrier, inc=1, device_id=place(k), device_id_type=pl.DeviceIdType.MESH
        )
        return carry

    lax.fori_loop(1, n, greet, 0)
    pl.semaphore_wait(barrier, n - 1)

    def copy(k):
        return pltpu.make_async_remote_copy(
            src_ref=own_ref,
            dst_ref=slots.at[k],
            send_sem=send_sem.at[k],
            recv_sem=recv_sem.at[k],
            device_id=place(k),
            device_id_type=pl.DeviceIdType.MESH,
        )

    def send(k, carry):
        copy(k).start()
        return carry

    lax.fori_loop(1, n, send, 0)

    def take(k, top):
        copy(k).wait_recv()
        return jnp.maximum(top, slots[k])

    out_ref[...] = lax.fori_loop(1, n, take, own_ref[...])

    def finish(k, carry):
        copy(k).wait_send()
        return carry

    lax.fori_loop(1, n, finish, 0)


def peak_everywhere(own):
    sizes = (lax.axis_size("gx"), lax.axis_size("gy"))
    n = sizes[0] * sizes[1]
    return pl.pallas_call(
        functools.partial(peak_kernel, sizes),
        out_shape=jax.ShapeDtypeStruct(own.shape, jnp.float32),
        in_specs=[VMEM],
        out_specs=VMEM,
        scratch_shapes=[
            pltpu.VMEM((n,) + own.shape, jnp.float32),
            pltpu.SemaphoreType.DMA((n,)),
            pltpu.SemaphoreType.DMA((n,)),
        ],
        compiler_params=pltpu.CompilerParams(collective_id=0, has_side_effects=True),
    )(own)


def move_kernel(scale_ref, v_ref, h_ref, qu_ref, qs_ref, target_ref, obstacle_ref, out_ref):
    planes, rows, cols, width = v_ref.shape

    def per_cell(i, carry):
        p, r = i // rows, i % rows
        change = scale_ref[0] * h_ref[p, r]
        change = change - scale_ref[1] * qu_ref[0, p, r] - scale_ref[2] * qs_ref[0, p, r]
        change = change - scale_ref[3] * qs_ref[1, p, r] - scale_ref[4] * qu_ref[1, p, r]
        change = change - scale_ref[5] * qu_ref[2, p, r]
        new = v_ref[p, r] - change
        new = jnp.where(target_ref[p, r] == 1, jnp.minimum(new, -0.5), new)
        out_ref[p, r] = jnp.where(obstacle_ref[p, r] == 1, jnp.maximum(new, 0.5), new)
        return carry

    lax.fori_loop(0, planes * rows, per_cell, 0)


VMEM = pl.BlockSpec(memory_space=pltpu.VMEM)
SMEM = pl.BlockSpec(memory_space=pltpu.SMEM)


def call(kernel, ins, outs, scratch, flops, args):
    return pl.pallas_call(
        kernel,
        out_shape=[jax.ShapeDtypeStruct(s, jnp.float32) for s in outs],
        in_specs=[SMEM] + [VMEM] * ins,
        out_specs=[VMEM] * len(outs),
        scratch_shapes=scratch,
        cost_estimate=pl.CostEstimate(flops=flops, bytes_accessed=1 << 20, transcendentals=0),
        compiler_params=pltpu.CompilerParams(vmem_limit_bytes=40 << 20),
    )(*args)


def drifts(shape, gains):
    planes, rows, cols, width = shape
    one = 2.0 * math.pi / (rows * lax.axis_size("gx"))
    two = 2.0 * math.pi / (cols * lax.axis_size("gy"))
    row = lax.axis_index("gx") * rows + jnp.arange(rows, dtype=jnp.int32)
    col = lax.axis_index("gy") * cols + jnp.arange(cols, dtype=jnp.int32)
    first = (jnp.arange(planes, dtype=jnp.float32) - planes / 2 + 0.5) * (2.0 / GRID)
    a = (one * row.astype(jnp.float32)).reshape(rows, 1, 1)
    b = (two * col.astype(jnp.float32)).reshape(1, cols, 1)
    lane = jnp.arange(width, dtype=jnp.int32)
    third = ((lane // N4).astype(jnp.float32) - N3 / 2 + 0.5) * (2.0 / GRID)
    fourth = ((lane % N4).astype(jnp.float32) - N4 / 2 + 0.5) * (2.0 / GRID)
    third, fourth = third.reshape(1, 1, -1), fourth.reshape(1, 1, -1)
    x0 = first.reshape(planes, 1, 1)
    f3 = gains[3] * (jnp.sin(b) - x0)
    return [
        gains[0] * (jnp.cos(a) - 0.5 * jnp.cos(b) + third),
        gains[1] * (fourth - 0.3 * x0),
        gains[2] * (third + 0.5 * jnp.sin(a)),
        jnp.broadcast_to(f3, (planes, cols, LANES)),
        gains[4] * (jnp.cos(a) * jnp.sin(b) - fourth),
    ]


def exchange(part_lo, part_hi, axis):
    devices = lax.axis_size(axis)
    up = [(i, (i + 1) % devices) for i in range(devices)]
    down = [(k, i) for i, k in up]
    return lax.ppermute(part_hi, axis, up), lax.ppermute(part_lo, axis, down)


def body(value, target, obstacle, gains, costs):
    shape = value.shape
    planes, rows, cols, width = shape
    h = jnp.array(
        [
            2.0 / GRID,
            2.0 * math.pi / (rows * lax.axis_size("gx")),
            2.0 * math.pi / (cols * lax.axis_size("gy")),
            2.0 / GRID,
            2.0 / GRID,
        ],
        dtype=jnp.float32,
    )
    kappa = costs / (288.0 * h)
    f = [d * (12.0 / costs[i]) for i, d in enumerate(drifts(shape, gains))]
    steps = []
    for _ in range(STEPS):
        a_lo, a_hi = exchange(value[:, :3], value[:, -3:], "gx")
        b_lo, b_hi = exchange(value[:, :, :3], value[:, :, -3:], "gy")
        part, q_un, peak_un = call(
            unsplit_kernel,
            4,
            [shape, (3,) + shape, (3, cols, width)],
            [pltpu.VMEM((12, planes, cols, width), jnp.float32)],
            1 << 28,
            (kappa, value, f[0], f[3], f[4]),
        )
        part, q_sp, top = call(
            split_kernel,
            9,
            [shape, (2,) + shape, (8, 128)],
            [
                pltpu.VMEM((cols + 6, width), jnp.float32),
                pltpu.VMEM((7, rows, cols, width), jnp.float32),
                pltpu.VMEM((2, cols, width), jnp.float32),
            ],
            1 << 27,
            (kappa, value, a_lo, a_hi, b_lo, b_hi, f[1], f[2], part, peak_un),
        )
        bounds = peak_everywhere(top)[:5, 0] * (costs / 12.0)
        dt = COURANT / (jnp.sum(bounds / h) + 1e-6)
        scales = jnp.concatenate([dt[None], dt * bounds / (12.0 * h)])
        (value,) = call(
            move_kernel, 6, [shape], [], 1 << 24,
            (scales, value, part, q_un, q_sp, target, obstacle),
        )
        steps.append(dt)
    return value, jnp.stack(steps)


def solution(mesh):
    spec = P(None, "gx", "gy", None)
    return jax.shard_map(
        body,
        mesh=mesh,
        in_specs=(spec, spec, spec, P(), P()),
        out_specs=(spec, P()),
        check_vma=False,
    )
```

```python
import functools
import math

import jax
import jax.numpy as jnp
from jax import lax
from jax.experimental import pallas as pl
from jax.experimental.pallas import tpu as pltpu
from jax.sharding import PartitionSpec as P

N3 = 32
N4 = 48
GRID = 96
STEPS = 3
COURANT = 0.5
EPS = 0.75e-6
LANES = 8 * N4


def wave(vs):
    n = len(vs) - 6
    d = [vs[k + 1] - vs[k] for k in range(n + 5)]
    f = [d[k + 1] - d[k] for k in range(n + 4)]
    e = [f[k + 1] - f[k] for k in range(n + 3)]
    j = [e[k + 1] - e[k] for k in range(n + 2)]
    k15 = [1.5 * x for x in f]
    base = [e[k] * e[k] + (0.5 * k15[k] * f[k + 1] + EPS) for k in range(n + 3)]
    left, mid, right = [], [], []
    for k in range(n + 1):
        a = base[k] + k15[k + 1] * e[k]
        b = base[k + 1]
        c = base[k + 2] - k15[k + 2] * e[k + 2]
        left.append(a * a)
        mid.append(b * b)
        right.append(c * c)
    low, high = [], []
    for k in range(n + 1):
        bc = mid[k] * right[k]
        ab = left[k] * mid[k]
        ac = 6.0 * (left[k] * right[k])
        n1 = bc * j[k]
        n2 = ab * j[k + 1]
        total = bc + ab
        both = n1 + n2
        both = both + both
        core = total + ac
        low.append((both + n2) / (core + (ab + ab)) if k < n else None)
        high.append((both + n1) / (core + (bc + bc)) if k > 0 else None)
    out = []
    for i in range(n):
        rm, rp = low[i], high[i + 1]
        center = 6.0 * (vs[i + 4] - vs[i + 2])
        middle = center - (e[i + 1] + e[i + 2]) + (rp - rm)
        jump = (rp + rm) - j[i + 1]
        out.append((middle, jump))
    return out


def tally(middle, jump, drift, kappa):
    gap = drift - middle
    return jnp.abs(gap) + jnp.abs(jump), (kappa * middle) * (drift + gap)


def unsplit_kernel(kappa_ref, v_ref, f0_ref, f3_ref, f4_ref, h_ref, q_ref, peak_ref, up_ref):
    planes, rows, cols, width = v_ref.shape
    lane = lax.broadcasted_iota(jnp.int32, (1, width), 1)
    third, fourth = lane // N4, lane % N4
    peak_ref[...] = jnp.zeros_like(peak_ref)

    def per_row(r, carry):
        def shift(p, carry):
            v = v_ref[p, r]
            for base, stride, place, extent in ((0, N4, third, width // N4), (6, 1, fourth, N4)):
                now = v
                for s in range(1, 4):
                    now = jnp.where(place + s < extent, pltpu.roll(v, width - s * stride, 1), now)
                    up_ref[base + 2 + s, p] = now
                now = v
                for s in range(1, 4):
                    now = jnp.where(place >= s, pltpu.roll(v, s * stride, 1), now)
                    up_ref[base + 3 - s, p] = now
            return carry

        lax.fori_loop(0, planes, shift, 0)

        def along_planes(g, carry):
            at = pl.ds(pl.multiple_of(g * 128, 128), 128)
            vs = [v_ref[p, r, :, at] for p in range(planes)]
            drift = f0_ref[r, :, at]
            top = peak_ref[0, :, at]
            cells = wave([vs[0]] * 3 + vs + [vs[-1]] * 3)
            for p in range(planes):
                speed, part = tally(*cells[p], drift, kappa_ref[0])
                top = jnp.maximum(top, speed)
                h_ref[p, r, :, at] = part
                q_ref[0, p, r, :, at] = cells[p][1]
            peak_ref[0, :, at] = top
            return carry

        lax.fori_loop(0, width // 128, along_planes, 0)

        def per_group(g, carry):
            at = pl.ds(pl.multiple_of(g * LANES, 128), LANES)

            def per_plane(p, carry):
                v = v_ref[p, r, :, at]
                total = h_ref[p, r, :, at]
                for slot, base, number in ((1, 0, 3), (2, 6, 4)):
                    around = [up_ref[base + k, p, :, at] for k in range(6)]
                    ((middle, jump),) = wave(around[:3] + [v] + around[3:])
                    drift = f3_ref[p, :, :] if number == 3 else f4_ref[r, :, at]
                    speed, part = tally(middle, jump, drift, kappa_ref[number])
                    peak_ref[slot, :, at] = jnp.maximum(peak_ref[slot, :, at], speed)
                    q_ref[slot, p, r, :, at] = jump
                    total = total + part
                h_ref[p, r, :, at] = total
                return carry

            lax.fori_loop(0, planes, per_plane, 0)
            return carry

        lax.fori_loop(0, width // LANES, per_group, 0)
        return carry

    lax.fori_loop(0, rows, per_row, 0)


def split_kernel(
    kappa_ref, v_ref, a_lo, a_hi, b_lo, b_hi, f1_ref, f2_ref, hin_ref, peak_un_ref,
    h_ref, q_ref, top_ref, ext_ref, near_ref, peak_ref,
):
    planes, rows, cols, width = v_ref.shape
    peak_ref[...] = jnp.zeros_like(peak_ref)

    def per_plane(p, carry):
        def fill(r, carry):
            ext_ref[0:3, :] = b_lo[p, r]
            ext_ref[3 : 3 + cols, :] = v_ref[p, r]
            ext_ref[3 + cols : 6 + cols, :] = b_hi[p, r]
            for k in range(7):
                near_ref[k, r] = ext_ref[k : k + cols, :]
            return carry

        lax.fori_loop(0, rows, fill, 0)

        def along_rows(g, carry):
            at = pl.ds(pl.multiple_of(g * 128, 128), 128)
            vs = [a_lo[p, k, :, at] for k in range(3)]
            vs += [v_ref[p, r, :, at] for r in range(rows)]
            vs += [a_hi[p, k, :, at] for k in range(3)]
            top = peak_ref[0, :, at]
            drift = f1_ref[p, :, at]
            for r, (middle, jump) in enumerate(wave(vs)):
                speed, part = tally(middle, jump, drift, kappa_ref[1])
                top = jnp.maximum(top, speed)
                h_ref[p, r, :, at] = hin_ref[p, r, :, at] + part
                q_ref[0, p, r, :, at] = jump
            peak_ref[0, :, at] = top
            return carry

        lax.fori_loop(0, width // 128, along_rows, 0)

        def per_group(g, carry):
            at = pl.ds(pl.multiple_of(g * LANES, 128), LANES)

            def per_row(r, carry):
                ((middle, jump),) = wave([near_ref[k, r, :, at] for k in range(7)])
                speed, part = tally(middle, jump, f2_ref[r, :, at], kappa_ref[2])
                peak_ref[1, :, at] = jnp.maximum(peak_ref[1, :, at], speed)
                h_ref[p, r, :, at] = h_ref[p, r, :, at] + part
                q_ref[1, p, r, :, at] = jump
                return carry

            lax.fori_loop(0, rows, per_row, 0)
            return carry

        lax.fori_loop(0, width // LANES, per_group, 0)
        return carry

    lax.fori_loop(0, planes, per_plane, 0)
    tops = [peak_un_ref[0], peak_ref[0], peak_ref[1], peak_un_ref[1], peak_un_ref[2]]
    row = lax.broadcasted_iota(jnp.int32, top_ref.shape, 0)
    out = jnp.zeros(top_ref.shape, jnp.float32)
    for number, part in enumerate(tops):
        out = jnp.where(row == number, jnp.max(part), out)
    top_ref[...] = out


def peak_kernel(axis, n, own_ref, out_ref, slots, send_sem, recv_sem):
    x, y = lax.axis_index("gx"), lax.axis_index("gy")

    def place(k):
        return ((x + k) % n, y) if axis == "gx" else (x, (y + k) % n)

    barrier = pltpu.get_barrier_semaphore()

    def greet(k, carry):
        pl.semaphore_signal(
            barrier, inc=1, device_id=place(k), device_id_type=pl.DeviceIdType.MESH
        )
        return carry

    lax.fori_loop(1, n, greet, 0)
    pl.semaphore_wait(barrier, n - 1)

    def copy(k):
        return pltpu.make_async_remote_copy(
            src_ref=own_ref,
            dst_ref=slots.at[k],
            send_sem=send_sem.at[k],
            recv_sem=recv_sem.at[k],
            device_id=place(k),
            device_id_type=pl.DeviceIdType.MESH,
        )

    def send(k, carry):
        copy(k).start()
        return carry

    lax.fori_loop(1, n, send, 0)

    def take(k, top):
        copy(k).wait_recv()
        return jnp.maximum(top, slots[k])

    out_ref[...] = lax.fori_loop(1, n, take, own_ref[...])

    def finish(k, carry):
        copy(k).wait_send()
        return carry

    lax.fori_loop(1, n, finish, 0)


def peak_along(own, axis, number):
    n = lax.axis_size(axis)
    return pl.pallas_call(
        functools.partial(peak_kernel, axis, n),
        out_shape=jax.ShapeDtypeStruct(own.shape, jnp.float32),
        in_specs=[VMEM],
        out_specs=VMEM,
        scratch_shapes=[
            pltpu.VMEM((n,) + own.shape, jnp.float32),
            pltpu.SemaphoreType.DMA((n,)),
            pltpu.SemaphoreType.DMA((n,)),
        ],
        compiler_params=pltpu.CompilerParams(collective_id=number, has_side_effects=True),
    )(own)


def move_kernel(scale_ref, v_ref, h_ref, qu_ref, qs_ref, target_ref, obstacle_ref, out_ref):
    planes, rows, cols, width = v_ref.shape

    def per_cell(i, carry):
        p, r = i // rows, i % rows
        change = scale_ref[0] * h_ref[p, r]
        change = change - scale_ref[1] * qu_ref[0, p, r] - scale_ref[2] * qs_ref[0, p, r]
        change = change - scale_ref[3] * qs_ref[1, p, r] - scale_ref[4] * qu_ref[1, p, r]
        change = change - scale_ref[5] * qu_ref[2, p, r]
        new = v_ref[p, r] - change
        new = jnp.where(target_ref[p, r] == 1, jnp.minimum(new, -0.5), new)
        out_ref[p, r] = jnp.where(obstacle_ref[p, r] == 1, jnp.maximum(new, 0.5), new)
        return carry

    lax.fori_loop(0, planes * rows, per_cell, 0)


VMEM = pl.BlockSpec(memory_space=pltpu.VMEM)
SMEM = pl.BlockSpec(memory_space=pltpu.SMEM)


def call(kernel, ins, outs, scratch, flops, args):
    return pl.pallas_call(
        kernel,
        out_shape=[jax.ShapeDtypeStruct(s, jnp.float32) for s in outs],
        in_specs=[SMEM] + [VMEM] * ins,
        out_specs=[VMEM] * len(outs),
        scratch_shapes=scratch,
        cost_estimate=pl.CostEstimate(flops=flops, bytes_accessed=1 << 20, transcendentals=0),
        compiler_params=pltpu.CompilerParams(vmem_limit_bytes=40 << 20),
    )(*args)


def drifts(shape, gains):
    planes, rows, cols, width = shape
    one = 2.0 * math.pi / (rows * lax.axis_size("gx"))
    two = 2.0 * math.pi / (cols * lax.axis_size("gy"))
    row = lax.axis_index("gx") * rows + jnp.arange(rows, dtype=jnp.int32)
    col = lax.axis_index("gy") * cols + jnp.arange(cols, dtype=jnp.int32)
    first = (jnp.arange(planes, dtype=jnp.float32) - planes / 2 + 0.5) * (2.0 / GRID)
    a = (one * row.astype(jnp.float32)).reshape(rows, 1, 1)
    b = (two * col.astype(jnp.float32)).reshape(1, cols, 1)
    lane = jnp.arange(width, dtype=jnp.int32)
    third = ((lane // N4).astype(jnp.float32) - N3 / 2 + 0.5) * (2.0 / GRID)
    fourth = ((lane % N4).astype(jnp.float32) - N4 / 2 + 0.5) * (2.0 / GRID)
    third, fourth = third.reshape(1, 1, -1), fourth.reshape(1, 1, -1)
    x0 = first.reshape(planes, 1, 1)
    f3 = gains[3] * (jnp.sin(b) - x0)
    return [
        gains[0] * (jnp.cos(a) - 0.5 * jnp.cos(b) + third),
        gains[1] * (fourth - 0.3 * x0),
        gains[2] * (third + 0.5 * jnp.sin(a)),
        jnp.broadcast_to(f3, (planes, cols, LANES)),
        gains[4] * (jnp.cos(a) * jnp.sin(b) - fourth),
    ]


def exchange(part_lo, part_hi, axis):
    devices = lax.axis_size(axis)
    up = [(i, (i + 1) % devices) for i in range(devices)]
    down = [(k, i) for i, k in up]
    return lax.ppermute(part_hi, axis, up), lax.ppermute(part_lo, axis, down)


def body(value, target, obstacle, gains, costs):
    shape = value.shape
    planes, rows, cols, width = shape
    h = jnp.array(
        [
            2.0 / GRID,
            2.0 * math.pi / (rows * lax.axis_size("gx")),
            2.0 * math.pi / (cols * lax.axis_size("gy")),
            2.0 / GRID,
            2.0 / GRID,
        ],
        dtype=jnp.float32,
    )
    kappa = costs / (288.0 * h)
    f = [d * (12.0 / costs[i]) for i, d in enumerate(drifts(shape, gains))]
    steps = []
    for _ in range(STEPS):
        a_lo, a_hi = exchange(value[:, :3], value[:, -3:], "gx")
        b_lo, b_hi = exchange(value[:, :, :3], value[:, :, -3:], "gy")
        part, q_un, peak_un = call(
            unsplit_kernel,
            4,
            [shape, (3,) + shape, (3, cols, width)],
            [pltpu.VMEM((12, planes, cols, width), jnp.float32)],
            1 << 28,
            (kappa, value, f[0], f[3], f[4]),
        )
        part, q_sp, top = call(
            split_kernel,
            9,
            [shape, (2,) + shape, (8, 128)],
            [
                pltpu.VMEM((cols + 6, width), jnp.float32),
                pltpu.VMEM((7, rows, cols, width), jnp.float32),
                pltpu.VMEM((2, cols, width), jnp.float32),
            ],
            1 << 27,
            (kappa, value, a_lo, a_hi, b_lo, b_hi, f[1], f[2], part, peak_un),
        )
        top = peak_along(peak_along(top, "gy", 0), "gx", 1)
        bounds = top[:5, 0] * (costs / 12.0)
        dt = COURANT / (jnp.sum(bounds / h) + 1e-6)
        scales = jnp.concatenate([dt[None], dt * bounds / (12.0 * h)])
        (value,) = call(
            move_kernel, 6, [shape], [], 1 << 24,
            (scales, value, part, q_un, q_sp, target, obstacle),
        )
        steps.append(dt)
    return value, jnp.stack(steps)


def solution(mesh):
    spec = P(None, "gx", "gy", None)
    return jax.shard_map(
        body,
        mesh=mesh,
        in_specs=(spec, spec, spec, P(), P()),
        out_specs=(spec, P()),
        check_vma=False,
    )
```
